32 devices in a mesh: cell: 16 (over z, y, core), band: 2 (over x).
Axes of the slice: x: 2, y: 2, z: 4, core: 2. Of those that a mesh axis runs over, the one named last changes fastest.
Arguments:
- positions: bfloat16 [32, 3, 96, 192], P('cell', None, 'band'), may hold values from -6 to 6
- densities: bfloat16 [32, 3, 96, 192], P('cell', None, 'band'), may hold values from -6 to 6
- operator: bfloat16 [640, 96, 192], P('cell', 'band'), may hold values from -0.046875 to 0.046875
- target_shift: int32 [32, 16], P('cell'), may hold values from 0 to 191
- weights: float32 [640], replicated, may hold values from 0.02 to 0.2
Outputs:
- velocity: float32 [32, 3, 16], P('cell')
The draws below stay inside these ranges and needn't reach their ends.
All inputs are finite; a program needn't handle non-finite values.
Results may differ from the reference program's by a relative error of at most 0.0003.
Values may be sent and summed in bfloat16 or wider, within the bound.
A program may use at most 64 MiB of HBM per device.

```python
import math
import jax
import jax.numpy as jnp
from jax import lax

LAT = 96
LON = 192
ROT = 640
TGT = 16
CAPS = 32


def set_ends(values, own_key, smallest, largest):
    spot = [jax.random.randint(jax.random.fold_in(own_key, axis), (), 0, length) for axis, length in enumerate(values.shape)]
    longest = values.shape.index(max(values.shape))
    neighbour = spot[:longest] + [(spot[longest] + 1) % values.shape[longest]] + spot[longest + 1:]
    return values.at[tuple(spot)].set(smallest).at[tuple(neighbour)].set(largest)


def shard_levels(own_key, shape, split, low, top_value):
    level, own = 1.0, jax.random.fold_in(own_key, 6)
    for position, shards_of in split:
        draws = jnp.exp(jax.random.uniform(jax.random.fold_in(own, position), (shards_of,), jnp.float32, low / len(split), top_value / len(split)))
        level = level * jnp.repeat(draws, shape[position] // shards_of).reshape([-1 if axis == position else 1 for axis in range(len(shape))])
    return level


def bell_draw(rng, extent, scale, most, shards=(), held_as=jnp.bfloat16):
    array = scale * jax.random.normal(rng, extent, jnp.float32)
    if shards:
        array = array * shard_levels(rng, extent, shards, -0.22, 0.18)
    return jnp.clip(array, -most, most).astype(held_as)


def setup_inputs(seed: int = 0) -> dict:
    seeds = jax.random.split(jax.random.key(seed), 6)
    positions = bell_draw(seeds[0], (CAPS, 3, LAT, LON), 1.0, 6.0, ((0, 16), (2, 2)))
    densities = bell_draw(seeds[1], (CAPS, 3, LAT, LON), 1.0, 6.0, ((0, 16), (2, 2)))
    operator = bell_draw(seeds[2], (ROT, LAT, LON), (LAT * LON) ** -0.5, 0.046875, ((0, 16), (1, 2)))
    target_shift = set_ends(jax.random.randint(seeds[3], (CAPS, TGT), 0, LON), jax.random.fold_in(seeds[3], 1), 0, LON - 1).astype(jnp.int32)
    weights = jnp.clip(jnp.exp(jax.random.uniform(seeds[4], (ROT,), jnp.float32, math.log(0.02), math.log(0.2))), 0.02, 0.2)
    return dict(positions=positions, densities=densities, operator=operator, target_shift=target_shift, weights=weights)


blob_radius = 0.5


def stokes(target, rows, weights):
    spread = target[:, :, :, None] - rows[:, 0:3]
    force = rows[:, 3:6]
    dist_sq = jnp.sum(spread * spread, axis=1)
    along = jnp.sum(spread * force, axis=1)
    blob_sq = blob_radius * blob_radius
    numer = (dist_sq + 2.0 * blob_sq)[:, None] * force + along[:, None] * spread
    kernel = weights / (dist_sq + blob_sq) ** 1.5
    return jnp.sum(numer * kernel[:, None], axis=-1)


def reference(positions, densities, operator, target_shift, weights):
    op_rows = operator.reshape(ROT, LAT * LON)

    def one_capsule(triple):
        posit, dense, shifts = triple
        source = jnp.concatenate([posit, dense], axis=0)
        indices = (jnp.arange(LON, dtype=jnp.int32)[None, :] + shifts[:, None]) % LON
        rolled = jnp.take(source, indices, axis=2)
        rolled = jnp.transpose(rolled, (0, 2, 1, 3)).reshape(6 * TGT, LAT * LON)
        result = lax.dot_general(rolled, op_rows, (((1,), (1,)), ((), ())), preferred_element_type=jnp.float32)
        return result.reshape(6, TGT, ROT)

    rotated = lax.map(one_capsule, (positions, densities, target_shift))
    return stokes(rotated[:, 0:3, :, 0], rotated, weights)
```

```python
import functools

import jax
import jax.numpy as jnp
from jax import lax
from jax.experimental import pallas as pl
from jax.experimental.pallas import tpu as pltpu
from jax.sharding import PartitionSpec as P

blob_radius = 0.5
MESH = pl.DeviceIdType.MESH
LANES = 128
GROUP = 8


def kernel(dims, src_ref, shift_ref, op_ref, weight_ref, out_ref, srcbuf, shiftbuf, opbuf,
           rolled, acc, xbuf, x0buf, vbuf, fin, src_send, src_recv, shift_send, shift_recv,
           op_send, op_recv, own_sem, x_send, x_recv, x0_send, x0_recv, fin_send, fin_recv):
    nz, nq, nb, caps, targets, pairs, rows, rows_pad, lon, chunks = dims
    cell, band = lax.axis_index("cell"), lax.axis_index("band")
    z, q = cell // nq, cell % nq
    depth = opbuf.shape[2]
    step = depth // chunks
    span = targets * GROUP
    keep = nz * caps // nb
    src_rows = pairs * GROUP
    side = q + 1 - 2 * (q % 2)
    across = (q + 2) % nq

    def cell_of(zz, qq):
        return zz * nq + qq

    barrier = pltpu.get_barrier_semaphore()
    for dz in range(nz):
        for db in range(nb):
            if dz or db:
                pl.semaphore_signal(barrier, inc=1, device_id=(cell_of((z + dz) % nz, q), (band + db) % nb), device_id_type=MESH)
    pl.semaphore_signal(barrier, inc=1, device_id=(cell_of(z, side), band), device_id_type=MESH)
    pl.semaphore_signal(barrier, inc=1, device_id=(cell_of(z, across), band), device_id_type=MESH)
    own = [pltpu.make_async_copy(src_ref, srcbuf.at[z], own_sem.at[0]),
           pltpu.make_async_copy(shift_ref, shiftbuf.at[z], own_sem.at[1]),
           pltpu.make_async_copy(op_ref, opbuf.at[q], own_sem.at[2])]
    for copy in own:
        copy.start()
    pl.semaphore_wait(barrier, nz * nb - 1 + 2)

    def op_copy(source, slot, part, target, lane):
        return pltpu.make_async_remote_copy(
            src_ref=source, dst_ref=opbuf.at[slot, :, pl.ds(part * step, step)],
            send_sem=op_send.at[lane, part], recv_sem=op_recv.at[lane, part],
            device_id=(cell_of(z, target), band), device_id_type=MESH)

    def src_copy(origin, dz):
        return pltpu.make_async_remote_copy(
            src_ref=src_ref, dst_ref=srcbuf.at[origin], send_sem=src_send.at[dz], recv_sem=src_recv.at[dz],
            device_id=(cell_of((z + dz) % nz, q), band), device_id_type=MESH)

    def shift_copy(origin, dz):
        return pltpu.make_async_remote_copy(
            src_ref=shift_ref, dst_ref=shiftbuf.at[origin], send_sem=shift_send.at[dz], recv_sem=shift_recv.at[dz],
            device_id=(cell_of((z + dz) % nz, q), band), device_id_type=MESH)

    to_across = [op_copy(op_ref.at[:, pl.ds(p * step, step)], q, p, across, 0) for p in range(chunks)]
    to_side = [op_copy(op_ref.at[:, pl.ds(p * step, step)], q, p, side, 1) for p in range(chunks)]
    forward = [op_copy(opbuf.at[across, :, pl.ds(p * step, step)], across, p, side, 2) for p in range(chunks)]
    order = [dz for d in range(1, nz // 2 + 1) for dz in ((d, nz - d) if d != nz - d else (d,))]
    for copy in to_across:
        copy.start()
    for dz in order:
        shift_copy(z, dz).start()
        src_copy(z, dz).start()
    for copy in to_side:
        copy.start()

    def roll(zz):
        lane_code = lax.broadcasted_iota(jnp.int32, (3 * LANES, 2 * LANES), 0)
        low = lon - LANES
        lane_code = jnp.where(lane_code < lon, lane_code,
                              jnp.where(lane_code < 2 * LANES, lane_code + 2 * low, lane_code - low))
        lane = lax.broadcasted_iota(jnp.int32, (1, LANES), 1)

        def wrap(value):
            return jnp.where(value >= lon, value - lon, value)

        def body(index, carry):
            cap, pair = index // (targets // 2), index % (targets // 2)
            goal = [[], [], []]
            for side_t in range(2):
                shift = shiftbuf[zz, pl.ds(cap * targets + pair * 2 + side_t, 1), :]
                first = wrap(lane + shift)
                goal[0].append(first)
                goal[1].append(first + lon)
                goal[2].append(jnp.where(lane < low, wrap(wrap(lane + LANES + shift - 0)), wrap(wrap(lane + LANES - low + shift)) + lon))
            base = pl.multiple_of(cap * src_rows, src_rows)
            for tile in range(3):
                wanted = jnp.concatenate(goal[tile], axis=1)
                begin, end = ((0, 2), (1, 3), (0, 3))[tile]
                hit = lane_code[begin * LANES:end * LANES] == wanted
                pick = jnp.where(hit, 1.0, 0.0).astype(jnp.bfloat16)
                moved = jnp.dot(srcbuf[zz, pl.ds(base, src_rows), begin * LANES:end * LANES], pick,
                                preferred_element_type=jnp.float32)
                row = pl.multiple_of((cap * nz + zz) * span + pair * 2 * GROUP, 2 * GROUP)
                for p in range(pairs):
                    both = jnp.concatenate([moved[p * GROUP:(p + 1) * GROUP, :LANES],
                                            moved[p * GROUP:(p + 1) * GROUP, LANES:]], axis=0)
                    rolled[pl.ds(row, 2 * GROUP), pl.ds((p * 3 + tile) * LANES, LANES)] = both.astype(jnp.bfloat16)
            return carry

        lax.fori_loop(0, caps * targets // 2, body, 0)

    own[0].wait()
    own[1].wait()
    roll(z)
    sent = 0
    for dz in order:
        zz = (z + nz - dz) % nz
        shift_copy(zz, dz).wait_recv()
        src_copy(zz, dz).wait_recv()
        roll(zz)
        if sent < chunks - 1:
            to_across[sent].wait_recv()
            forward[sent].start()
            sent += 1
    while sent < chunks:
        to_across[sent].wait_recv()
        forward[sent].start()
        sent += 1
    own[2].wait()
    for copy in to_side:
        copy.wait_recv()

    for p in range(chunks):
        forward[p].wait_recv()
        blocks = opbuf[:, :, pl.ds(p * step, step)].reshape(nq * rows_pad, step)

        def multiply(index, carry):
            at = pl.multiple_of(index * 2 * span, 2 * span)
            part = lax.dot_general(blocks, rolled[pl.ds(at, 2 * span), pl.ds(p * step, step)],
                                   (((1,), (1,)), ((), ())), preferred_element_type=jnp.float32)
            for half in range(2):
                where = index * 2 + half
                piece = part[:, half * span:(half + 1) * span]
                if p == 0:
                    acc[where] = piece
                else:
                    acc[where] += piece
            return carry

        lax.fori_loop(0, nz * caps // 2, multiply, 0)

    def x_copy(db, block, origin):
        target = (band + db) % nb
        return pltpu.make_async_remote_copy(
            src_ref=acc.at[pl.ds(target * keep, keep), pl.ds(block * rows_pad, rows_send), :],
            dst_ref=xbuf.at[origin, :, pl.ds(block * rows_pad, rows_send), :],
            send_sem=x_send.at[db, block], recv_sem=x_recv.at[db, block],
            device_id=(cell, target), device_id_type=MESH)

    rows_send = (rows + GROUP - 1) // GROUP * GROUP
    for db in range(1, nb):
        for block in range(nq):
            x_copy(db, block, band).start()
    for db in range(1, nb):
        for block in range(nq):
            x_copy(db, block, (band + nb - db) % nb).wait_recv()

    def total(i, block):
        value = acc[band * keep + i, block * rows_pad:block * rows_pad + rows_send, :]
        for db in range(1, nb):
            value = value + xbuf[(band + nb - db) % nb, i, block * rows_pad:block * rows_pad + rows_send, :]
        return value

    def x0_copy(dz):
        return pltpu.make_async_remote_copy(
            src_ref=x0buf, dst_ref=x0buf, send_sem=x0_send.at[dz], recv_sem=x0_recv.at[0],
            device_id=(cell_of(dz, q), band), device_id_type=MESH)

    @pl.when(z == 0)
    def _():
        for i in range(keep):
            x0buf[i] = total(i, 0)[0:GROUP]
        for dz in range(1, nz):
            x0_copy(dz).start()

    @pl.when(z != 0)
    def _():
        x0_copy(1).wait_recv()

    lane = lax.broadcasted_iota(jnp.int32, (1, span), 1) % GROUP
    blob_sq = blob_radius * blob_radius

    def fin_copy(i, x, origin_cap, origin_z):
        return pltpu.make_async_remote_copy(
            src_ref=vbuf.at[i], dst_ref=fin.at[origin_cap, origin_z], send_sem=fin_send.at[i, x],
            recv_sem=fin_recv.at[origin_cap, origin_z],
            device_id=(cell_of((band * keep + i) % nz, q), x), device_id_type=MESH)

    def three(value):
        value = jnp.where(lane < 3, value, 0.0)
        value = value + pltpu.roll(value, 1, 1) + pltpu.roll(value, 2, 1)
        value = jnp.where(lane == 2, value, 0.0)
        return value + pltpu.roll(value, span - 1, 1) + pltpu.roll(value, span - 2, 1)

    for i in range(keep):
        velocity = jnp.zeros((GROUP, span), jnp.float32)
        for block in range(nq):
            value = total(i, block)
            spread = x0buf[i, 0:1] - value
            force = pltpu.roll(value, span - 3, 1)
            dist_sq = three(spread * spread)
            along = three(spread * force)
            inverse = lax.rsqrt(dist_sq + blob_sq)
            share = weight_ref[block * rows_pad:block * rows_pad + rows_send, :] * (inverse * inverse * inverse)
            term = ((dist_sq + 2.0 * blob_sq) * force + along * spread) * share
            term = jnp.where(lane < 3, term, 0.0)
            for k in range(rows_send // GROUP):
                velocity = velocity + term[k * GROUP:(k + 1) * GROUP]
        vbuf[i] = velocity
        g = band * keep + i
        for x in range(nb):
            itself = jnp.logical_and(g % nz == z, band == x)

            @pl.when(itself)
            def _():
                fin[g // nz, z] = velocity

            @pl.when(jnp.logical_not(itself))
            def _():
                fin_copy(i, x, g // nz, z).start()

    for cap in range(caps):
        for zz in range(nz):
            itself = jnp.logical_and(z == zz, (cap * nz + z) // keep == band)

            @pl.when(jnp.logical_not(itself))
            def _():
                fin_copy(0, 0, cap, zz).wait_recv()

    out_ref[...] = jnp.zeros_like(out_ref)
    for cap in range(caps):
        value = fin[cap, 0]
        for zz in range(1, nz):
            value = value + fin[cap, zz]
        out_ref[cap:cap + 1, :] = jnp.sum(value, axis=0, keepdims=True)

    for copy in to_across + to_side + forward:
        copy.wait_send()
    for dz in order:
        shift_copy(z, dz).wait_send()
        src_copy(z, dz).wait_send()
    for db in range(1, nb):
        for block in range(nq):
            x_copy(db, block, band).wait_send()

    @pl.when(z == 0)
    def _():
        for dz in range(1, nz):
            x0_copy(dz).wait_send()

    for i in range(keep):
        for x in range(nb):
            itself = jnp.logical_and((band * keep + i) % nz == z, band == x)

            @pl.when(jnp.logical_not(itself))
            def _():
                fin_copy(i, x, 0, 0).wait_send()


def per_device(cells, bands, positions, densities, operator, target_shift, weights):
    caps, comps, lat, lon = positions.shape
    targets = target_shift.shape[1]
    rows = operator.shape[0]
    nq = 4
    nz = cells // nq
    pairs = lat // 2
    rows_pad = (rows + 15) // 16 * 16
    rows_send = (rows + 7) // 8 * 8
    depth = lat * lon
    chunks = 4 if (depth // LANES) % 4 == 0 else 2
    span = targets * GROUP
    keep = nz * caps // bands

    def tiles(array):
        lead = array.shape[:-2]
        high = array[..., :LANES].reshape(lead + (pairs, 2, LANES))
        low = array[..., LANES:].reshape(lead + (pairs, LANES))
        return high[..., 0, :], high[..., 1, :], low

    first, second, low = tiles(operator)
    op = jnp.stack([first, second, low], axis=2).reshape(rows, depth)
    op = jnp.pad(op, ((0, rows_pad - rows), (0, 0)))
    source = jnp.concatenate([positions, densities], axis=1)
    source = jnp.pad(source, ((0, 0), (0, GROUP - 2 * comps), (0, 0), (0, 0)))
    source = jnp.transpose(source.reshape(caps, GROUP, pairs, 2, lon), (0, 2, 1, 3, 4))
    first, second = source[..., 0, :], source[..., 1, :]
    source = jnp.concatenate([first, second[..., LANES:], second[..., :LANES]], axis=-1)
    source = source.reshape(caps * pairs * GROUP, 3 * LANES)
    shifts = jnp.broadcast_to(target_shift.reshape(caps * targets, 1), (caps * targets, LANES))
    z = lax.axis_index("cell") // nq
    mine = lax.dynamic_slice(weights, (z * nq * rows,), (nq * rows,)).reshape(nq, rows)
    mine = jnp.pad(mine, ((0, 0), (0, rows_pad - rows))).reshape(nq * rows_pad, 1)
    mine = jnp.broadcast_to(mine, (nq * rows_pad, span))
    dims = (nz, nq, bands, caps, targets, pairs, rows, rows_pad, lon, chunks)
    dma = pltpu.SemaphoreType.DMA
    hbm = pl.BlockSpec(memory_space=pl.ANY)
    vmem = pl.BlockSpec(memory_space=pltpu.VMEM)
    out = pl.pallas_call(
        functools.partial(kernel, dims),
        out_shape=jax.ShapeDtypeStruct((GROUP, span), jnp.float32),
        in_specs=[hbm, hbm, hbm, vmem],
        out_specs=vmem,
        scratch_shapes=[
            pltpu.VMEM((nz,) + source.shape, jnp.bfloat16),
            pltpu.VMEM((nz, caps * targets, LANES), jnp.int32),
            pltpu.VMEM((nq, rows_pad, depth), jnp.bfloat16),
            pltpu.VMEM((nz * caps * span, depth), jnp.bfloat16),
            pltpu.VMEM((nz * caps, nq * rows_pad, span), jnp.float32),
            pltpu.VMEM((bands, keep, nq * rows_pad, span), jnp.float32),
            pltpu.VMEM((keep, GROUP, span), jnp.float32),
            pltpu.VMEM((keep, GROUP, span), jnp.float32),
            pltpu.VMEM((caps, nz, GROUP, span), jnp.float32),
            dma((nz,)), dma((nz,)), dma((nz,)), dma((nz,)),
            dma((3, chunks)), dma((3, chunks)), dma((3,)),
            dma((bands, nq)), dma((bands, nq)), dma((nz,)), dma((1,)),
            dma((keep, bands)), dma((caps, nz)),
        ],
        compiler_params=pltpu.CompilerParams(
            collective_id=0, has_side_effects=True, vmem_limit_bytes=60 * 1024 * 1024
        ),
    )(source, shifts, op, mine)
    velocity = out[:caps].reshape(caps, targets, GROUP)[:, :, :comps]
    return jnp.transpose(velocity, (0, 2, 1))


def solution(mesh):
    in_specs = (
        P("cell", None, "band", None),
        P("cell", None, "band", None),
        P("cell", "band", None),
        P("cell", None),
        P(),
    )
    out_specs = P("cell", None, None)
    body = functools.partial(per_device, mesh.shape["cell"], mesh.shape["band"])
    return jax.shard_map(body, mesh=mesh, in_specs=in_specs, out_specs=out_specs, check_vma=False)
```

```python
import functools

import jax
import jax.numpy as jnp
from jax import lax
from jax.experimental import pallas as pl
from jax.experimental.pallas import tpu as pltpu
from jax.sharding import PartitionSpec as P

blob_radius = 0.5
MESH = pl.DeviceIdType.MESH
LANES = 128
GROUP = 8


def kernel(dims, src_ref, shift_ref, op_ref, weight_ref, out_ref, srcbuf, shiftbuf, opbuf, wide,
           rolled, acc, xbuf, x0buf, vbuf, fin, src_send, src_recv, shift_send, shift_recv,
           op_send, op_recv, own_sem, x_send, x_recv, x0_send, x0_recv, fin_send, fin_recv):
    nz, nq, nb, caps, targets, pairs, rows, rows_pad, lon, chunks = dims
    cell, band = lax.axis_index("cell"), lax.axis_index("band")
    z, q = cell // nq, cell % nq
    depth = opbuf.shape[2]
    step = depth // chunks
    span = targets * GROUP
    keep = nz * caps // nb
    src_rows = pairs * GROUP
    comps = srcbuf.shape[2] // pairs
    side = q + 1 - 2 * (q % 2)
    across = (q + 2) % nq

    def cell_of(zz, qq):
        return zz * nq + qq

    barrier = pltpu.get_barrier_semaphore()
    for dz in range(nz):
        for db in range(nb):
            if dz or db:
                pl.semaphore_signal(barrier, inc=1, device_id=(cell_of((z + dz) % nz, q), (band + db) % nb), device_id_type=MESH)
    pl.semaphore_signal(barrier, inc=1, device_id=(cell_of(z, side), band), device_id_type=MESH)
    pl.semaphore_signal(barrier, inc=1, device_id=(cell_of(z, across), band), device_id_type=MESH)
    own = [pltpu.make_async_copy(src_ref, srcbuf.at[z], own_sem.at[0]),
           pltpu.make_async_copy(shift_ref, shiftbuf.at[z], own_sem.at[1]),
           pltpu.make_async_copy(op_ref, opbuf.at[q], own_sem.at[2])]
    for copy in own:
        copy.start()
    pl.semaphore_wait(barrier, nz * nb - 1 + 2)

    def op_copy(source, slot, part, target, lane):
        return pltpu.make_async_remote_copy(
            src_ref=source, dst_ref=opbuf.at[slot, :, pl.ds(part * step, step)],
            send_sem=op_send.at[lane, part], recv_sem=op_recv.at[lane, part],
            device_id=(cell_of(z, target), band), device_id_type=MESH)

    def line_copy(origin, way, first):
        lane = 2 * way + (0 if first else 1)
        target = (cell_of(z + 1 - 2 * way, q), band)
        return (pltpu.make_async_remote_copy(
            src_ref=shift_ref if first else shiftbuf.at[origin], dst_ref=shiftbuf.at[origin],
            send_sem=shift_send.at[lane, origin], recv_sem=shift_recv.at[origin],
            device_id=target, device_id_type=MESH), pltpu.make_async_remote_copy(
            src_ref=src_ref if first else srcbuf.at[origin], dst_ref=srcbuf.at[origin],
            send_sem=src_send.at[lane, origin], recv_sem=src_recv.at[origin],
            device_id=target, device_id_type=MESH))

    inner = (z < nz - 1, z > 0)

    to_across = [op_copy(op_ref.at[:, pl.ds(p * step, step)], q, p, across, 0) for p in range(chunks)]
    to_side = [op_copy(op_ref.at[:, pl.ds(p * step, step)], q, p, side, 1) for p in range(chunks)]
    forward = [op_copy(opbuf.at[across, :, pl.ds(p * step, step)], across, p, side, 2) for p in range(chunks)]
    for copy in to_across:
        copy.start()
    for way in range(2):
        @pl.when(inner[way])
        def _():
            for copy in line_copy(z, way, True):
                copy.start()
    for copy in to_side:
        copy.start()

    def roll(zz):
        lane_code = lax.broadcasted_iota(jnp.int32, (3 * LANES, 2 * LANES), 0)
        low = lon - LANES
        lane_code = jnp.where(lane_code < lon, lane_code,
                              jnp.where(lane_code < 2 * LANES, lane_code + 2 * low, lane_code - low))
        lane = lax.broadcasted_iota(jnp.int32, (1, LANES), 1)

        def wrap(value):
            return jnp.where(value >= lon, value - lon, value)

        grid = (src_rows, pairs * comps)
        at, of = lax.broadcasted_iota(jnp.int32, grid, 0), lax.broadcasted_iota(jnp.int32, grid, 1)
        spread_out = jnp.logical_and(at % GROUP < comps, of == at // GROUP * comps + at % GROUP)
        spread_out = jnp.where(spread_out, 1.0, 0.0).astype(jnp.bfloat16)
        for cap in range(caps):
            wide[cap * src_rows:(cap + 1) * src_rows, :] = jnp.dot(
                spread_out, srcbuf[zz, cap], preferred_element_type=jnp.float32).astype(jnp.bfloat16)

        def body(index, carry):
            cap, pair = index // (targets // 2), index % (targets // 2)
            goal = [[], [], []]
            for side_t in range(2):
                shift = shiftbuf[zz, pl.ds(cap * targets + pair * 2 + side_t, 1), :]
                first = wrap(lane + shift)
                goal[0].append(first)
                goal[1].append(first + lon)
                goal[2].append(jnp.where(lane < low, wrap(wrap(lane + LANES + shift - 0)), wrap(wrap(lane + LANES - low + shift)) + lon))
            base = pl.multiple_of(cap * src_rows, src_rows)
            for tile in range(3):
                wanted = jnp.concatenate(goal[tile], axis=1)
                begin, end = ((0, 2), (1, 3), (0, 3))[tile]
                hit = lane_code[begin * LANES:end * LANES] == wanted
                pick = jnp.where(hit, 1.0, 0.0).astype(jnp.bfloat16)
                moved = jnp.dot(wide[pl.ds(base, src_rows), begin * LANES:end * LANES], pick,
                                preferred_element_type=jnp.float32)
                row = pl.multiple_of((cap * nz + zz) * span + pair * 2 * GROUP, 2 * GROUP)
                for p in range(pairs):
                    both = jnp.concatenate([moved[p * GROUP:(p + 1) * GROUP, :LANES],
                                            moved[p * GROUP:(p + 1) * GROUP, LANES:]], axis=0)
                    rolled[pl.ds(row, 2 * GROUP), pl.ds((p * 3 + tile) * LANES, LANES)] = both.astype(jnp.bfloat16)
            return carry

        lax.fori_loop(0, caps * targets // 2, body, 0)

    own[0].wait()
    own[1].wait()
    roll(z)
    sent = 0
    for d in range(1, nz):
        for way in range(2):
            origin = (z - d, z + d)[way]
            there = (z >= d, z + d < nz)[way]

            @pl.when(there)
            def _():
                for copy in line_copy(origin, way, False):
                    copy.wait_recv()

            @pl.when(jnp.logical_and(there, inner[way]))
            def _():
                for copy in line_copy(origin, way, False):
                    copy.start()

        for way in range(2):
            origin = (z - d, z + d)[way]
            there = (z >= d, z + d < nz)[way]

            @pl.when(there)
            def _():
                roll(origin)
        if sent < chunks - 1:
            to_across[sent].wait_recv()
            forward[sent].start()
            sent += 1
    while sent < chunks:
        to_across[sent].wait_recv()
        forward[sent].start()
        sent += 1
    own[2].wait()
    for copy in to_side:
        copy.wait_recv()

    rows_send = (rows + GROUP - 1) // GROUP * GROUP

    def x_copy(db, block, origin):
        target = (band + db) % nb
        return pltpu.make_async_remote_copy(
            src_ref=acc.at[pl.ds(target * keep, keep), pl.ds(block * rows_pad, rows_send), :],
            dst_ref=xbuf.at[origin, :, pl.ds(block * rows_pad, rows_send), :],
            send_sem=x_send.at[db, block], recv_sem=x_recv.at[db, block],
            device_id=(cell, target), device_id_type=MESH)

    def multiply(p, begin, count):
        blocks = opbuf[:, :, pl.ds(p * step, step)].reshape(nq * rows_pad, step)

        def body(index, carry):
            first = begin + index * 2
            at = pl.multiple_of(first * span, 2 * span)
            part = lax.dot_general(blocks, rolled[pl.ds(at, 2 * span), pl.ds(p * step, step)],
                                   (((1,), (1,)), ((), ())), preferred_element_type=jnp.float32)
            for half in range(2):
                piece = part[:, half * span:(half + 1) * span]
                if p == 0:
                    acc[first + half] = piece
                else:
                    acc[first + half] += piece
            return carry

        lax.fori_loop(0, count // 2, body, 0)

    for p in range(chunks):
        forward[p].wait_recv()
        if p < chunks - 1:
            multiply(p, 0, nz * caps)
        else:
            for db in range(1, nb + 1):
                multiply(p, (band + db) % nb * keep, keep)
                if db < nb:
                    for block in range(nq):
                        x_copy(db, block, band).start()

    def await_block(block):
        for db in range(1, nb):
            x_copy(db, block, (band + nb - db) % nb).wait_recv()

    def total(block):
        value = acc[pl.ds(band * keep, keep), block * rows_pad:block * rows_pad + rows_send, :]
        for db in range(1, nb):
            value = value + xbuf[(band + nb - db) % nb, :, block * rows_pad:block * rows_pad + rows_send, :]
        return value

    def x0_copy(dz):
        return pltpu.make_async_remote_copy(
            src_ref=x0buf, dst_ref=x0buf, send_sem=x0_send.at[dz], recv_sem=x0_recv.at[0],
            device_id=(cell_of(dz, q), band), device_id_type=MESH)

    await_block(0)

    @pl.when(z == 0)
    def _():
        x0buf[...] = total(0)[:, 0:GROUP, :]
        for dz in range(1, nz):
            x0_copy(dz).start()

    for block in range(1, nq):
        await_block(block)

    @pl.when(z != 0)
    def _():
        x0_copy(1).wait_recv()

    lane = lax.broadcasted_iota(jnp.int32, (1, span), 1) % GROUP
    blob_sq = blob_radius * blob_radius

    def fin_copy(i, x, origin_cap, origin_z):
        return pltpu.make_async_remote_copy(
            src_ref=vbuf.at[i], dst_ref=fin.at[origin_cap, origin_z], send_sem=fin_send.at[i, x],
            recv_sem=fin_recv.at[origin_cap, origin_z],
            device_id=(cell_of((band * keep + i) % nz, q), x), device_id_type=MESH)

    def turn(value, amount):
        return pltpu.roll(value, amount % span, 1)

    def three(value):
        value = jnp.where(lane < 3, value, 0.0)
        value = value + turn(value, 1) + turn(value, 2)
        value = jnp.where(lane == 2, value, 0.0)
        return value + turn(value, -1) + turn(value, -2)

    velocities = jnp.zeros((keep, GROUP, span), jnp.float32)
    pole = x0buf[:, 0:1, :]
    for block in range(nq):
        value = total(block)
        spread = (pole - value).reshape(keep * rows_send, span)
        force = turn(value.reshape(keep * rows_send, span), -3)
        dist_sq = three(spread * spread)
        along = three(spread * force)
        inverse = lax.rsqrt(dist_sq + blob_sq)
        term = ((dist_sq + 2.0 * blob_sq) * force + along * spread) * (inverse * inverse * inverse)
        term = jnp.where(lane < 3, term, 0.0).reshape(keep, rows_send, span)
        term = term * weight_ref[z * nq + block, 0:rows_send, :]
        for k in range(rows_send // GROUP):
            velocities = velocities + term[:, k * GROUP:(k + 1) * GROUP]

    for i in range(keep):
        velocity = velocities[i]
        vbuf[i] = velocity
        g = band * keep + i
        for x in range(nb):
            itself = jnp.logical_and(g % nz == z, band == x)

            @pl.when(itself)
            def _():
                fin[g // nz, z] = velocity

            @pl.when(jnp.logical_not(itself))
            def _():
                fin_copy(i, x, g // nz, z).start()

    for cap in range(caps):
        for zz in range(nz):
            itself = jnp.logical_and(z == zz, (cap * nz + z) // keep == band)

            @pl.when(jnp.logical_not(itself))
            def _():
                fin_copy(0, 0, cap, zz).wait_recv()

    out_ref[...] = jnp.zeros_like(out_ref)
    for cap in range(caps):
        value = fin[cap, 0]
        for zz in range(1, nz):
            value = value + fin[cap, zz]
        out_ref[cap:cap + 1, :] = jnp.sum(value, axis=0, keepdims=True)

    for copy in to_across + to_side + forward:
        copy.wait_send()
    for way in range(2):
        @pl.when(inner[way])
        def _():
            for copy in line_copy(z, way, True):
                copy.wait_send()
    for d in range(1, nz):
        for way in range(2):
            origin = (z - d, z + d)[way]
            there = (z >= d, z + d < nz)[way]

            @pl.when(jnp.logical_and(there, inner[way]))
            def _():
                for copy in line_copy(origin, way, False):
                    copy.wait_send()
    for db in range(1, nb):
        for block in range(nq):
            x_copy(db, block, band).wait_send()

    @pl.when(z == 0)
    def _():
        for dz in range(1, nz):
            x0_copy(dz).wait_send()

    for i in range(keep):
        for x in range(nb):
            itself = jnp.logical_and((band * keep + i) % nz == z, band == x)

            @pl.when(jnp.logical_not(itself))
            def _():
                fin_copy(i, x, 0, 0).wait_send()


def per_device(cells, bands, positions, densities, operator, target_shift, weights):
    caps, comps, lat, lon = positions.shape
    targets = target_shift.shape[1]
    rows = operator.shape[0]
    nq = 4
    nz = cells // nq
    pairs = lat // 2
    rows_pad = (rows + 15) // 16 * 16
    rows_send = (rows + 7) // 8 * 8
    depth = lat * lon
    chunks = 4 if (depth // LANES) % 4 == 0 else 2
    span = targets * GROUP
    keep = nz * caps // bands

    def tiles(array):
        lead = array.shape[:-2]
        high = array[..., :LANES].reshape(lead + (pairs, 2, LANES))
        low = array[..., LANES:].reshape(lead + (pairs, LANES))
        return high[..., 0, :], high[..., 1, :], low

    first, second, low = tiles(operator)
    op = jnp.stack([first, second, low], axis=2).reshape(rows, depth)
    op = jnp.pad(op, ((0, rows_pad - rows), (0, 0)))
    source = jnp.concatenate([positions, densities], axis=1)
    source = jnp.transpose(source.reshape(caps, 2 * comps, pairs, 2, lon), (0, 2, 1, 3, 4))
    first, second = source[..., 0, :], source[..., 1, :]
    source = jnp.concatenate([first, second[..., LANES:], second[..., :LANES]], axis=-1)
    source = source.reshape(caps, pairs * 2 * comps, 3 * LANES)
    shifts = jnp.broadcast_to(target_shift.reshape(caps * targets, 1), (caps * targets, LANES))
    mine = weights.reshape(cells, rows, 1)
    mine = jnp.pad(mine, ((0, 0), (0, rows_pad - rows), (0, 0)))
    dims = (nz, nq, bands, caps, targets, pairs, rows, rows_pad, lon, chunks)
    dma = pltpu.SemaphoreType.DMA
    hbm = pl.BlockSpec(memory_space=pl.ANY)
    vmem = pl.BlockSpec(memory_space=pltpu.VMEM)
    out = pl.pallas_call(
        functools.partial(kernel, dims),
        out_shape=jax.ShapeDtypeStruct((GROUP, span), jnp.float32),
        in_specs=[hbm, hbm, hbm, vmem],
        out_specs=vmem,
        scratch_shapes=[
            pltpu.VMEM((nz,) + source.shape, jnp.bfloat16),
            pltpu.VMEM((nz, caps * targets, LANES), jnp.int32),
            pltpu.VMEM((nq, rows_pad, depth), jnp.bfloat16),
            pltpu.VMEM((caps * pairs * GROUP, 3 * LANES), jnp.bfloat16),
            pltpu.VMEM((nz * caps * span, depth), jnp.bfloat16),
            pltpu.VMEM((nz * caps, nq * rows_pad, span), jnp.float32),
            pltpu.VMEM((bands, keep, nq * rows_pad, span), jnp.float32),
            pltpu.VMEM((keep, GROUP, span), jnp.float32),
            pltpu.VMEM((keep, GROUP, span), jnp.float32),
            pltpu.VMEM((caps, nz, GROUP, span), jnp.float32),
            dma((4, nz)), dma((nz,)), dma((4, nz)), dma((nz,)),
            dma((3, chunks)), dma((3, chunks)), dma((3,)),
            dma((bands, nq)), dma((bands, nq)), dma((nz,)), dma((1,)),
            dma((keep, bands)), dma((caps, nz)),
        ],
        compiler_params=pltpu.CompilerParams(
            collective_id=0, has_side_effects=True, vmem_limit_bytes=60 * 1024 * 1024
        ),
    )(source, shifts, op, mine)
    velocity = out[:caps].reshape(caps, targets, GROUP)[:, :, :comps]
    return jnp.transpose(velocity, (0, 2, 1))


def solution(mesh):
    in_specs = (
        P("cell", None, "band", None),
        P("cell", None, "band", None),
        P("cell", "band", None),
        P("cell", None),
        P(),
    )
    out_specs = P("cell", None, None)
    body = functools.partial(per_device, mesh.shape["cell"], mesh.shape["band"])
    return jax.shard_map(body, mesh=mesh, in_specs=in_specs, out_specs=out_specs, check_vma=False)
```

```python
import functools

import jax
import jax.numpy as jnp
from jax import lax
from jax.experimental import pallas as pl
from jax.experimental.pallas import tpu as pltpu
from jax.sharding import PartitionSpec as P

blob_radius = 0.5
MESH = pl.DeviceIdType.MESH
LANES = 128
GROUP = 8


def kernel(dims, src_ref, shift_ref, op_ref, weight_ref, out_ref, srcbuf, shiftbuf, opbuf, wide,
           rolled, acc, xbuf, x0buf, vbuf, fin, src_send, src_recv, shift_send, shift_recv,
           op_send, op_recv, own_sem, x_send, x_recv, x0_send, x0_recv, fin_send, fin_recv):
    nz, nq, nb, caps, targets, pairs, rows, rows_pad, lon, chunks = dims
    cell, band = lax.axis_index("cell"), lax.axis_index("band")
    z, q = cell // nq, cell % nq
    depth = opbuf.shape[2]
    step = depth // chunks
    span = targets * GROUP
    keep = nz * caps // nb
    src_rows = pairs * GROUP
    comps = srcbuf.shape[2] // pairs
    side = q + 1 - 2 * (q % 2)
    across = (q + 2) % nq

    def cell_of(zz, qq):
        return zz * nq + qq

    barrier = pltpu.get_barrier_semaphore()
    for dz in range(nz):
        for db in range(nb):
            if dz or db:
                pl.semaphore_signal(barrier, inc=1, device_id=(cell_of((z + dz) % nz, q), (band + db) % nb), device_id_type=MESH)
    pl.semaphore_signal(barrier, inc=1, device_id=(cell_of(z, side), band), device_id_type=MESH)
    pl.semaphore_signal(barrier, inc=1, device_id=(cell_of(z, across), band), device_id_type=MESH)
    own = [pltpu.make_async_copy(src_ref, srcbuf.at[z], own_sem.at[0]),
           pltpu.make_async_copy(shift_ref, shiftbuf.at[z], own_sem.at[1]),
           pltpu.make_async_copy(op_ref, opbuf.at[q], own_sem.at[2])]
    for copy in own:
        copy.start()
    pl.semaphore_wait(barrier, nz * nb - 1 + 2)

    def op_copy(source, slot, part, target, lane):
        return pltpu.make_async_remote_copy(
            src_ref=source, dst_ref=opbuf.at[slot, :, pl.ds(part * step, step)],
            send_sem=op_send.at[lane, part], recv_sem=op_recv.at[lane, part],
            device_id=(cell_of(z, target), band), device_id_type=MESH)

    def line_copy(origin, way, first):
        lane = 2 * way + (0 if first else 1)
        target = (cell_of(z + 1 - 2 * way, q), band)
        return (pltpu.make_async_remote_copy(
            src_ref=shift_ref if first else shiftbuf.at[origin], dst_ref=shiftbuf.at[origin],
            send_sem=shift_send.at[lane, origin], recv_sem=shift_recv.at[origin],
            device_id=target, device_id_type=MESH), pltpu.make_async_remote_copy(
            src_ref=src_ref if first else srcbuf.at[origin], dst_ref=srcbuf.at[origin],
            send_sem=src_send.at[lane, origin], recv_sem=src_recv.at[origin],
            device_id=target, device_id_type=MESH))

    inner = (z < nz - 1, z > 0)

    to_across = [op_copy(op_ref.at[:, pl.ds(p * step, step)], q, p, across, 0) for p in range(chunks)]
    to_side = [op_copy(op_ref.at[:, pl.ds(p * step, step)], q, p, side, 1) for p in range(chunks)]
    forward = [op_copy(opbuf.at[across, :, pl.ds(p * step, step)], across, p, side, 2) for p in range(chunks)]
    for copy in to_across:
        copy.start()
    for way in range(2):
        @pl.when(inner[way])
        def _():
            for copy in line_copy(z, way, True):
                copy.start()
    for copy in to_side:
        copy.start()

    def roll(zz):
        lane_code = lax.broadcasted_iota(jnp.int32, (3 * LANES, 2 * LANES), 0)
        low = lon - LANES
        lane_code = jnp.where(lane_code < lon, lane_code,
                              jnp.where(lane_code < 2 * LANES, lane_code + 2 * low, lane_code - low))
        lane = lax.broadcasted_iota(jnp.int32, (1, LANES), 1)

        def wrap(value):
            return jnp.where(value >= lon, value - lon, value)

        grid = (src_rows, pairs * comps)
        at, of = lax.broadcasted_iota(jnp.int32, grid, 0), lax.broadcasted_iota(jnp.int32, grid, 1)
        spread_out = jnp.logical_and(at % GROUP < comps, of == at // GROUP * comps + at % GROUP)
        spread_out = jnp.where(spread_out, 1.0, 0.0).astype(jnp.bfloat16)
        for cap in range(caps):
            wide[cap * src_rows:(cap + 1) * src_rows, :] = jnp.dot(
                spread_out, srcbuf[zz, cap], preferred_element_type=jnp.float32).astype(jnp.bfloat16)

        def body(index, carry):
            cap, pair = index // (targets // 2), index % (targets // 2)
            goal = [[], [], []]
            for side_t in range(2):
                shift = shiftbuf[zz, pl.ds(cap * targets + pair * 2 + side_t, 1), :]
                first = wrap(lane + shift)
                goal[0].append(first)
                goal[1].append(first + lon)
                goal[2].append(jnp.where(lane < low, wrap(wrap(lane + LANES + shift - 0)), wrap(wrap(lane + LANES - low + shift)) + lon))
            base = pl.multiple_of(cap * src_rows, src_rows)
            for tile in range(3):
                wanted = jnp.concatenate(goal[tile], axis=1)
                begin, end = ((0, 2), (1, 3), (0, 3))[tile]
                hit = lane_code[begin * LANES:end * LANES] == wanted
                pick = jnp.where(hit, 1.0, 0.0).astype(jnp.bfloat16)
                moved = jnp.dot(wide[pl.ds(base, src_rows), begin * LANES:end * LANES], pick,
                                preferred_element_type=jnp.float32)
                row = pl.multiple_of((cap * nz + zz) * span + pair * 2 * GROUP, 2 * GROUP)
                for p in range(pairs):
                    both = jnp.concatenate([moved[p * GROUP:(p + 1) * GROUP, :LANES],
                                            moved[p * GROUP:(p + 1) * GROUP, LANES:]], axis=0)
                    rolled[pl.ds(row, 2 * GROUP), pl.ds((p * 3 + tile) * LANES, LANES)] = both.astype(jnp.bfloat16)
            return carry

        def twice(index, carry):
            return body(index * 2 + 1, body(index * 2, carry))

        lax.fori_loop(0, caps * targets // 4, twice, 0)

    own[0].wait()
    own[1].wait()
    roll(z)
    sent = 0
    for d in range(1, nz):
        for way in range(2):
            origin = (z - d, z + d)[way]
            there = (z >= d, z + d < nz)[way]

            @pl.when(there)
            def _():
                for copy in line_copy(origin, way, False):
                    copy.wait_recv()

            @pl.when(jnp.logical_and(there, inner[way]))
            def _():
                for copy in line_copy(origin, way, False):
                    copy.start()

        for way in range(2):
            origin = (z - d, z + d)[way]
            there = (z >= d, z + d < nz)[way]

            @pl.when(there)
            def _():
                roll(origin)
        if sent < chunks - 1:
            to_across[sent].wait_recv()
            forward[sent].start()
            sent += 1
    while sent < chunks:
        to_across[sent].wait_recv()
        forward[sent].start()
        sent += 1
    own[2].wait()
    for copy in to_side:
        copy.wait_recv()

    rows_send = (rows + GROUP - 1) // GROUP * GROUP

    def x_copy(db, block, origin):
        target = (band + db) % nb
        return pltpu.make_async_remote_copy(
            src_ref=acc.at[pl.ds(target * keep, keep), pl.ds(block * rows_pad, rows_send), :],
            dst_ref=xbuf.at[origin, :, pl.ds(block * rows_pad, rows_send), :],
            send_sem=x_send.at[db, block], recv_sem=x_recv.at[db, block],
            device_id=(cell, target), device_id_type=MESH)

    def multiply(p, begin, count):
        blocks = opbuf[:, :, pl.ds(p * step, step)].reshape(nq * rows_pad, step)

        def body(index, carry):
            first = begin + index * 2
            at = pl.multiple_of(first * span, 2 * span)
            part = lax.dot_general(blocks, rolled[pl.ds(at, 2 * span), pl.ds(p * step, step)],
                                   (((1,), (1,)), ((), ())), preferred_element_type=jnp.float32)
            for half in range(2):
                piece = part[:, half * span:(half + 1) * span]
                if p == 0:
                    acc[first + half] = piece
                else:
                    acc[first + half] += piece
            return carry

        def twice(index, carry):
            return body(index * 2 + 1, body(index * 2, carry))

        lax.fori_loop(0, count // 4, twice, 0)

    for p in range(chunks):
        forward[p].wait_recv()
        if p < chunks - 1:
            multiply(p, 0, nz * caps)
        else:
            for db in range(1, nb + 1):
                multiply(p, (band + db) % nb * keep, keep)
                if db < nb:
                    for block in range(nq):
                        x_copy(db, block, band).start()

    def await_block(block):
        for db in range(1, nb):
            x_copy(db, block, (band + nb - db) % nb).wait_recv()

    def total(block):
        value = acc[pl.ds(band * keep, keep), block * rows_pad:block * rows_pad + rows_send, :]
        for db in range(1, nb):
            value = value + xbuf[(band + nb - db) % nb, :, block * rows_pad:block * rows_pad + rows_send, :]
        return value

    def x0_copy(dz):
        return pltpu.make_async_remote_copy(
            src_ref=x0buf, dst_ref=x0buf, send_sem=x0_send.at[dz], recv_sem=x0_recv.at[0],
            device_id=(cell_of(dz, q), band), device_id_type=MESH)

    await_block(0)

    @pl.when(z == 0)
    def _():
        x0buf[...] = total(0)[:, 0:GROUP, :]
        for dz in range(1, nz):
            x0_copy(dz).start()

    for block in range(1, nq):
        await_block(block)

    @pl.when(z != 0)
    def _():
        x0_copy(1).wait_recv()

    lane = lax.broadcasted_iota(jnp.int32, (1, span), 1) % GROUP
    blob_sq = blob_radius * blob_radius

    def fin_copy(i, x, origin_cap, origin_z):
        return pltpu.make_async_remote_copy(
            src_ref=vbuf.at[i], dst_ref=fin.at[origin_cap, origin_z], send_sem=fin_send.at[i, x],
            recv_sem=fin_recv.at[origin_cap, origin_z],
            device_id=(cell_of((band * keep + i) % nz, q), x), device_id_type=MESH)

    def turn(value, amount):
        return pltpu.roll(value, amount % span, 1)

    def three(value):
        value = jnp.where(lane < 3, value, 0.0)
        value = value + turn(value, 1) + turn(value, 2)
        value = jnp.where(lane == 2, value, 0.0)
        return value + turn(value, -1) + turn(value, -2)

    velocities = jnp.zeros((keep, GROUP, span), jnp.float32)
    pole = x0buf[:, 0:1, :]
    for block in range(nq):
        value = total(block)
        spread = (pole - value).reshape(keep * rows_send, span)
        force = turn(value.reshape(keep * rows_send, span), -3)
        dist_sq = three(spread * spread)
        along = three(spread * force)
        inverse = lax.rsqrt(dist_sq + blob_sq)
        term = ((dist_sq + 2.0 * blob_sq) * force + along * spread) * (inverse * inverse * inverse)
        term = jnp.where(lane < 3, term, 0.0).reshape(keep, rows_send, span)
        term = term * weight_ref[z * nq + block, 0:rows_send, :]
        for k in range(rows_send // GROUP):
            velocities = velocities + term[:, k * GROUP:(k + 1) * GROUP]

    for i in range(keep):
        velocity = velocities[i]
        vbuf[i] = velocity
        g = band * keep + i
        for x in range(nb):
            itself = jnp.logical_and(g % nz == z, band == x)

            @pl.when(itself)
            def _():
                fin[g // nz, z] = velocity

            @pl.when(jnp.logical_not(itself))
            def _():
                fin_copy(i, x, g // nz, z).start()

    for cap in range(caps):
        for zz in range(nz):
            itself = jnp.logical_and(z == zz, (cap * nz + z) // keep == band)

            @pl.when(jnp.logical_not(itself))
            def _():
                fin_copy(0, 0, cap, zz).wait_recv()

    out_ref[...] = jnp.zeros_like(out_ref)
    for cap in range(caps):
        value = fin[cap, 0]
        for zz in range(1, nz):
            value = value + fin[cap, zz]
        out_ref[cap:cap + 1, :] = jnp.sum(value, axis=0, keepdims=True)

    for copy in to_across + to_side + forward:
        copy.wait_send()
    for way in range(2):
        @pl.when(inner[way])
        def _():
            for copy in line_copy(z, way, True):
                copy.wait_send()
    for d in range(1, nz):
        for way in range(2):
            origin = (z - d, z + d)[way]
            there = (z >= d, z + d < nz)[way]

            @pl.when(jnp.logical_and(there, inner[way]))
            def _():
                for copy in line_copy(origin, way, False):
                    copy.wait_send()
    for db in range(1, nb):
        for block in range(nq):
            x_copy(db, block, band).wait_send()

    @pl.when(z == 0)
    def _():
        for dz in range(1, nz):
            x0_copy(dz).wait_send()

    for i in range(keep):
        for x in range(nb):
            itself = jnp.logical_and((band * keep + i) % nz == z, band == x)

            @pl.when(jnp.logical_not(itself))
            def _():
                fin_copy(i, x, 0, 0).wait_send()


def per_device(cells, bands, positions, densities, operator, target_shift, weights):
    caps, comps, lat, lon = positions.shape
    targets = target_shift.shape[1]
    rows = operator.shape[0]
    nq = 4
    nz = cells // nq
    pairs = lat // 2
    rows_pad = (rows + 15) // 16 * 16
    rows_send = (rows + 7) // 8 * 8
    depth = lat * lon
    chunks = 4 if (depth // LANES) % 4 == 0 else 2
    span = targets * GROUP
    keep = nz * caps // bands

    def tiles(array):
        lead = array.shape[:-2]
        high = array[..., :LANES].reshape(lead + (pairs, 2, LANES))
        low = array[..., LANES:].reshape(lead + (pairs, LANES))
        return high[..., 0, :], high[..., 1, :], low

    first, second, low = tiles(operator)
    op = jnp.stack([first, second, low], axis=2).reshape(rows, depth)
    op = jnp.pad(op, ((0, rows_pad - rows), (0, 0)))
    source = jnp.concatenate([positions, densities], axis=1)
    source = jnp.transpose(source.reshape(caps, 2 * comps, pairs, 2, lon), (0, 2, 1, 3, 4))
    first, second = source[..., 0, :], source[..., 1, :]
    source = jnp.concatenate([first, second[..., LANES:], second[..., :LANES]], axis=-1)
    source = source.reshape(caps, pairs * 2 * comps, 3 * LANES)
    shifts = jnp.broadcast_to(target_shift.reshape(caps * targets, 1), (caps * targets, LANES))
    mine = weights.reshape(cells, rows, 1)
    mine = jnp.pad(mine, ((0, 0), (0, rows_pad - rows), (0, 0)))
    dims = (nz, nq, bands, caps, targets, pairs, rows, rows_pad, lon, chunks)
    dma = pltpu.SemaphoreType.DMA
    hbm = pl.BlockSpec(memory_space=pl.ANY)
    vmem = pl.BlockSpec(memory_space=pltpu.VMEM)
    out = pl.pallas_call(
        functools.partial(kernel, dims),
        out_shape=jax.ShapeDtypeStruct((GROUP, span), jnp.float32),
        in_specs=[hbm, hbm, hbm, vmem],
        out_specs=vmem,
        scratch_shapes=[
            pltpu.VMEM((nz,) + source.shape, jnp.bfloat16),
            pltpu.VMEM((nz, caps * targets, LANES), jnp.int32),
            pltpu.VMEM((nq, rows_pad, depth), jnp.bfloat16),
            pltpu.VMEM((caps * pairs * GROUP, 3 * LANES), jnp.bfloat16),
            pltpu.VMEM((nz * caps * span, depth), jnp.bfloat16),
            pltpu.VMEM((nz * caps, nq * rows_pad, span), jnp.float32),
            pltpu.VMEM((bands, keep, nq * rows_pad, span), jnp.float32),
            pltpu.VMEM((keep, GROUP, span), jnp.float32),
            pltpu.VMEM((keep, GROUP, span), jnp.float32),
            pltpu.VMEM((caps, nz, GROUP, span), jnp.float32),
            dma((4, nz)), dma((nz,)), dma((4, nz)), dma((nz,)),
            dma((3, chunks)), dma((3, chunks)), dma((3,)),
            dma((bands, nq)), dma((bands, nq)), dma((nz,)), dma((1,)),
            dma((keep, bands)), dma((caps, nz)),
        ],
        compiler_params=pltpu.CompilerParams(
            collective_id=0, has_side_effects=True, vmem_limit_bytes=60 * 1024 * 1024
        ),
    )(source, shifts, op, mine)
    velocity = out[:caps].reshape(caps, targets, GROUP)[:, :, :comps]
    return jnp.transpose(velocity, (0, 2, 1))


def solution(mesh):
    in_specs = (
        P("cell", None, "band", None),
        P("cell", None, "band", None),
        P("cell", "band", None),
        P("cell", None),
        P(),
    )
    out_specs = P("cell", None, None)
    body = functools.partial(per_device, mesh.shape["cell"], mesh.shape["band"])
    return jax.shard_map(body, mesh=mesh, in_specs=in_specs, out_specs=out_specs, check_vma=False)
```
